32 devices in a mesh: ctx: 8 (over y, x, core), tp: 4 (over z).
Axes of the slice: x: 2, y: 2, z: 4, core: 2. Of those that a mesh axis runs over, the one named last changes fastest.
Arguments:
- resid: bfloat16 [16384, 4096], P('ctx', 'tp'), may hold values from -6 to 6
- sel_blocks: int32 [16], P('ctx'), may hold values from 0 to 127, as said below
- norm_gain: float32 [4096], replicated, may hold values from 0.5 to 1.5
- router_weight: float32 [4096], replicated, may hold values from -0.09375 to 0.09375
- w_query: bfloat16 [4096, 4096], P(None, 'tp'), may hold values from -0.25 to 0.25
- w_key: bfloat16 [4096, 512], P(None, 'tp'), may hold values from -4 to 4
- value_projection: bfloat16 [4096, 512], P(None, 'tp'), may hold values from -0.09375 to 0.09375
- w_out: bfloat16 [4096, 4096], P('tp'), may hold values from -0.09375 to 0.09375
Outputs:
- mixed: bfloat16 [2048, 4096], P(('ctx', 'tp'))
The draws below stay inside these ranges and needn't reach their ends.
Inputs may be any that keep to these rules, and one draw needn't show every extreme that they name: `sel_blocks`: entries 2 * c to 2 * c + 1 are 2 different numbers from c * 16 to c * 16 + 15, increasing.
All inputs are finite; a program needn't handle non-finite values.
Results may differ from the reference program's by a relative error of at most 0.0075.
Values may be sent and summed in bfloat16 or wider, within the bound.
A program may use at most 128 MiB of HBM per device.

```python
import math
import jax
import jax.numpy as jnp
from jax import lax

MODEL_WIDTH = 4096
HEAD_WIDTH = 128
KEY_VALUE_HEADS = 4
QUERY_GROUP_SIZE = 8
BLK = 128
NBLK_DEV = 16
HQ = 32
SEL_DEV = 2
TOKENS = 16384
NBLK = 128
SELECTED_ROWS = 2048


def pick_blocks(key):
    devices = NBLK // NBLK_DEV
    scores = jax.random.randint(key, (devices, NBLK_DEV), 0, 1 << 20) * NBLK_DEV + jnp.arange(NBLK_DEV, dtype=jnp.int32)[None, :]
    unused, picked = lax.top_k(scores, SEL_DEV)
    picked = jnp.sort(picked, axis=1)
    return (picked + jnp.arange(devices, dtype=jnp.int32)[:, None] * NBLK_DEV).reshape(devices * SEL_DEV).astype(jnp.int32)


def draw_sel_blocks(key, part):
    return pick_blocks(jax.random.fold_in(key, 3))


def attention_weights(key):
    base_key = jax.random.fold_in(key, 7)
    initial_random_key, middle_random_key = jax.random.split(base_key, 2)
    query_lookup_table = jax.random.normal(initial_random_key, (MODEL_WIDTH, KEY_VALUE_HEADS, QUERY_GROUP_SIZE, HEAD_WIDTH), jnp.float32) / math.sqrt(MODEL_WIDTH)
    key_lookup_table = 3.0 * jax.random.normal(middle_random_key, (MODEL_WIDTH, KEY_VALUE_HEADS, HEAD_WIDTH), jnp.float32) / math.sqrt(MODEL_WIDTH)
    query_lookup_table = jnp.clip(query_lookup_table, -0.25, 0.25).reshape(MODEL_WIDTH, HQ * HEAD_WIDTH)
    key_lookup_table = jnp.clip(key_lookup_table, -4.0, 4.0).reshape(MODEL_WIDTH, KEY_VALUE_HEADS * HEAD_WIDTH)
    return (query_lookup_table, key_lookup_table)


def draw_w_query(key, part):
    return attention_weights(key)[0].astype(jnp.bfloat16)


def draw_w_key(key, part):
    return attention_weights(key)[1].astype(jnp.bfloat16)


def level_of(key, dims, cuts, smallest, top_value):
    def one(dim, blocks):
        draws = jax.random.uniform(jax.random.fold_in(jax.random.fold_in(key, 6), dim), (blocks,), jnp.float32, smallest / len(cuts), top_value / len(cuts))
        return jnp.repeat(jnp.exp(draws), dims[dim] // blocks).reshape((-1,) + (1,) * (len(dims) - dim - 1))

    factor_of = one(*cuts[0])
    for cut in cuts[1:]:
        factor_of = factor_of * one(*cut)
    return factor_of


def noise(stream_key, extent, width, bound, shards=(), held_as=jnp.bfloat16):
    factor_of = level_of(stream_key, extent, shards, -0.22, 0.18) if shards else 1.0
    array = jax.random.normal(stream_key, extent, jnp.float32) * width * factor_of
    return jnp.minimum(jnp.maximum(array, -bound), bound).astype(held_as)


def setup_inputs(seed: int = 0) -> dict:
    key_list = jax.random.split(jax.random.key(seed), 9)
    resid = noise(key_list[0], (TOKENS, MODEL_WIDTH), 1.0, 6.0, ((0, 8), (1, 4)))
    sel_blocks = draw_sel_blocks(jax.random.fold_in(key_list[8], 71), 0)
    norm_gain = jnp.clip(1.0 + 0.1 * jax.random.normal(key_list[2], (MODEL_WIDTH,), jnp.float32), 0.5, 1.5)
    router_weight = noise(key_list[3], (MODEL_WIDTH,), MODEL_WIDTH ** -0.5, 0.09375, (), jnp.float32)
    w_query = draw_w_query(jax.random.fold_in(key_list[8], 71), 0)
    w_key = draw_w_key(jax.random.fold_in(key_list[8], 71), 0)
    value_projection = noise(key_list[6], (MODEL_WIDTH, KEY_VALUE_HEADS * HEAD_WIDTH), MODEL_WIDTH ** -0.5, 0.09375, ((1, 4),))
    w_out = noise(key_list[7], (HQ * HEAD_WIDTH, MODEL_WIDTH), (HQ * HEAD_WIDTH) ** -0.5, 0.09375, ((0, 4),))
    return dict(resid=resid, sel_blocks=sel_blocks, norm_gain=norm_gain, router_weight=router_weight, w_query=w_query, w_key=w_key, value_projection=value_projection, w_out=w_out)


rope_base = 500000.0
norm_eps = 1e-05

def rotate_heads(values_in, positions, head_size):
    rows = values_in.shape[0]
    heads = values_in.shape[1] // head_size
    shaped = values_in.reshape(rows, heads, head_size)
    half_size = head_size // 2
    freqs = jnp.exp(jnp.arange(half_size, dtype=jnp.float32) * (-2.0 * math.log(rope_base) / head_size))
    angles = positions.astype(jnp.float32)[:, None] * freqs[None, :]
    cosine = jnp.cos(angles)[:, None, :]
    sine = jnp.sin(angles)[:, None, :]
    first = shaped[:, :, :half_size]
    second = shaped[:, :, half_size:]
    turned = jnp.concatenate([first * cosine - second * sine, second * cosine + first * sine], axis=2)
    return turned.reshape(rows, heads * head_size).astype(jnp.bfloat16)

def reference(resid, sel_blocks, norm_gain, router_weight, w_query, w_key, value_projection, w_out):
    position = (sel_blocks[:, None] * BLK + jnp.arange(BLK, dtype=jnp.int32)[None, :]).reshape(SELECTED_ROWS).astype(jnp.int32)
    chosen = resid[position]
    chosen_wide = chosen.astype(jnp.float32)
    inv_rms = lax.rsqrt(lax.optimization_barrier(jnp.mean(chosen_wide * chosen_wide, axis=1)) + norm_eps)
    normed = (chosen_wide * inv_rms[:, None] * norm_gain[None, :]).astype(jnp.bfloat16)
    gate = jax.nn.sigmoid(lax.optimization_barrier(jnp.sum(chosen_wide * router_weight[None, :], axis=1)))
    queries = rotate_heads(jnp.dot(normed, w_query, preferred_element_type=jnp.float32), position, HEAD_WIDTH)
    key_matrix = rotate_heads(jnp.dot(normed, w_key, preferred_element_type=jnp.float32), position, HEAD_WIDTH)
    value_matrix = jnp.dot(normed, value_projection, preferred_element_type=jnp.float32).astype(jnp.bfloat16)
    query_heads = queries.reshape(SELECTED_ROWS, HQ, HEAD_WIDTH).transpose(1, 0, 2)
    per_head_keys = key_matrix.reshape(SELECTED_ROWS, KEY_VALUE_HEADS, HEAD_WIDTH).transpose(1, 0, 2)
    per_head_values = value_matrix.reshape(SELECTED_ROWS, KEY_VALUE_HEADS, HEAD_WIDTH).transpose(1, 0, 2)
    allowed = position[None, :] <= position[:, None]
    score_scale = 1.0 / math.sqrt(HEAD_WIDTH)

    def one_head(head):
        query_one = query_heads[head]
        key_one = per_head_keys[head // QUERY_GROUP_SIZE]
        value_one = per_head_values[head // QUERY_GROUP_SIZE]
        scores = jnp.dot(query_one, key_one.T, preferred_element_type=jnp.float32) * score_scale
        scores = jnp.where(allowed, scores, -jnp.inf)
        highest = lax.optimization_barrier(jnp.max(scores, axis=1, keepdims=True))
        expd = jnp.exp(scores - highest)
        weights = expd.astype(jnp.bfloat16)
        mixed_values = jnp.dot(weights, value_one, preferred_element_type=jnp.float32)
        return (mixed_values / lax.optimization_barrier(jnp.sum(expd, axis=1, keepdims=True))).astype(jnp.bfloat16)
    per_head = lax.map(one_head, jnp.arange(HQ, dtype=jnp.int32))
    attended = per_head.transpose(1, 0, 2).reshape(SELECTED_ROWS, HQ * HEAD_WIDTH)
    projected = jnp.dot(attended, w_out, preferred_element_type=jnp.float32)
    return (chosen_wide + gate[:, None] * projected).astype(jnp.bfloat16)
```

```python
import functools
import math

import jax
import jax.numpy as jnp
import numpy as np
from jax import lax
from jax.experimental import pallas as pl
from jax.experimental.pallas import tpu as pltpu
from jax.sharding import PartitionSpec as P

HEAD_WIDTH = 128
BLK = 128
ROPE_BASE = 500000.0
NORM_EPS = 1e-05
MASKED = -1e30
MESH = pl.DeviceIdType.MESH
ROW_CHUNKS = 4
BF16 = jnp.bfloat16
F32 = jnp.float32


def pick(sel_ref, resid_hbm, row_hbm, block_hbm, x_ref, rot, row_ref, block_ref, sem):
    picked = x_ref.shape[0] // BLK
    total_blocks = block_ref.shape[0] // 2
    before = lax.axis_index("ctx") * (resid_hbm.shape[0] // BLK)
    copies = [
        pltpu.make_async_copy(
            resid_hbm.at[pl.ds(pl.multiple_of((sel_ref[i] - before) * BLK, BLK), BLK), :],
            x_ref.at[pl.ds(i * BLK, BLK), :],
            sem.at[i],
        )
        for i in range(picked)
    ]
    tables = [
        pltpu.make_async_copy(src, dst, sem.at[picked + i])
        for i, (src, dst) in enumerate(((row_hbm, row_ref), (block_hbm, block_ref)))
    ]
    for copy in copies + tables:
        copy.start()
    for copy in tables:
        copy.wait()
    hw = HEAD_WIDTH
    flip = jnp.where(lax.broadcasted_iota(jnp.int32, (1, hw), 1) < hw // 2, -1.0, 1.0)
    for i in range(picked):
        part = slice(i * BLK, (i + 1) * BLK)
        block_cos = block_ref[pl.ds(sel_ref[i], 1), :]
        block_sin = block_ref[pl.ds(sel_ref[i] + total_blocks, 1), :]
        row_cos, row_sin = row_ref[:BLK, :], row_ref[BLK:, :]
        rot[0, part, :] = block_cos * row_cos - block_sin * row_sin
        rot[1, part, :] = (block_sin * row_cos + block_cos * row_sin) * flip
    for copy in copies:
        copy.wait()


def fused(
    tp_size, ctx_size,
    x_hbm, rot_hbm, gain_hbm, router_hbm, wq_hbm, wk_hbm, wv_hbm, wo_hbm,
    out_ref,
    rot, gain_ref, router_ref, xg, wq, wkv, wo, qacc, kvacc, sumsq, qs, kvs, high, total, accum, att,
    sbuf, rbuf, fin,
    w_sem, ag_send, ag_recv, kv_send, kv_recv, rs_send, rs_recv,
):
    me = lax.axis_index("tp")
    c = lax.axis_index("ctx")
    rows, width = xg.shape[1:]
    heads = wq.shape[1] // HEAD_WIDTH
    hw = HEAD_WIDTH
    chunk = rows // ROW_CHUNKS
    share = rows // tp_size
    has_up = me < tp_size - 1
    has_dn = me > 0

    copies = [
        pltpu.make_async_copy(src, dst, w_sem.at[i])
        for i, (src, dst) in enumerate(
            (
                (x_hbm, xg.at[me]),
                (gain_hbm, gain_ref),
                (wk_hbm, wkv.at[:, pl.ds(0, hw)]),
                (wv_hbm, wkv.at[:, pl.ds(hw, hw)]),
                (wq_hbm, wq),
                (rot_hbm, rot),
                (wo_hbm, wo),
                (router_hbm, router_ref),
            )
        )
    ]
    for copy in copies:
        copy.start()

    barrier = pltpu.get_barrier_semaphore()

    @pl.when(has_up)
    def _():
        pl.semaphore_signal(barrier, inc=1, device_id={"tp": me + 1}, device_id_type=MESH)

    @pl.when(has_dn)
    def _():
        pl.semaphore_signal(barrier, inc=1, device_id={"tp": me - 1}, device_id_type=MESH)

    def greet(k, carry):
        peer = lax.rem(c + k, ctx_size)
        pl.semaphore_signal(barrier, inc=1, device_id={"ctx": peer}, device_id_type=MESH)
        return carry

    lax.fori_loop(1, ctx_size, greet, 0)
    copies[0].wait()
    pl.semaphore_wait(
        barrier, ctx_size - 1 + has_up.astype(jnp.int32) + has_dn.astype(jnp.int32)
    )

    def feature_copy(src, slot, q, direction):
        side = 0 if direction > 0 else 1
        part = pl.ds(q * chunk, chunk)
        return pltpu.make_async_remote_copy(
            src_ref=src.at[part, :],
            dst_ref=xg.at[slot, part, :],
            send_sem=ag_send.at[side, slot, q],
            recv_sem=ag_recv.at[slot, q],
            device_id={"tp": me + direction},
            device_id_type=MESH,
        )

    for q in range(ROW_CHUNKS):
        for direction, there in ((1, has_up), (-1, has_dn)):
            @pl.when(there)
            def _():
                feature_copy(xg.at[me], me, q, direction).start()

    sumsq[...] = jnp.zeros_like(sumsq)
    qacc[...] = jnp.zeros_like(qacc)
    kvacc[...] = jnp.zeros_like(kvacc)
    for i in (1, 2, 3):
        copies[i].wait()

    def project_kv(slot, part):
        depth = pl.ds(pl.multiple_of(slot * width, width), width)
        wide = xg[slot, part, :].astype(F32)
        sumsq[part, :] += jnp.sum(wide * wide, axis=1, keepdims=True)
        scaled = (wide * gain_ref[:, depth]).astype(BF16)
        kvacc[part, :] += jnp.dot(scaled, wkv[depth, :], preferred_element_type=F32)

    def project_q(slot):
        depth = pl.ds(pl.multiple_of(slot * width, width), width)
        scaled = (xg[slot].astype(F32) * gain_ref[:, depth]).astype(BF16)
        qacc[...] += jnp.dot(scaled, wq[depth, :], preferred_element_type=F32)

    def project_q_hop(h):
        for direction in (1, -1):
            slot = me - direction * h
            inside = jnp.logical_and(slot >= 0, slot < tp_size)

            @pl.when(jnp.logical_and(inside, jnp.logical_or(h > 0, direction > 0)))
            def _():
                project_q(slot)

    project_kv(me, slice(0, rows))
    copies[4].wait()
    halves = 2
    per_half = ROW_CHUNKS // halves

    def hop(h, carry):
        project_q_hop(h - 1)
        for q in range(ROW_CHUNKS):
            for direction, onward in ((1, has_up), (-1, has_dn)):
                slot = me - direction * h
                inside = jnp.logical_and(slot >= 0, slot < tp_size)

                @pl.when(inside)
                def _():
                    feature_copy(xg.at[slot], slot, q, direction).wait_recv()

                @pl.when(jnp.logical_and(inside, onward))
                def _():
                    feature_copy(xg.at[slot], slot, q, direction).start()

            if (q + 1) % per_half == 0:
                part = slice((q + 1 - per_half) * chunk, (q + 1) * chunk)
                for direction in (1, -1):
                    slot = me - direction * h

                    @pl.when(jnp.logical_and(slot >= 0, slot < tp_size))
                    def _():
                        project_kv(slot, part)

        return carry

    lax.fori_loop(1, tp_size - 1, hop, 0)
    project_q_hop(tp_size - 2)
    copies[5].wait()

    def kv_copy(slot, q, peer, send):
        part = pl.ds(q * chunk, chunk)
        return pltpu.make_async_remote_copy(
            src_ref=kvs.at[slot, part, :],
            dst_ref=kvs.at[slot, part, :],
            send_sem=send,
            recv_sem=kv_recv.at[slot, q],
            device_id={"ctx": peer},
            device_id_type=MESH,
        )

    last = tp_size - 1
    for q in range(ROW_CHUNKS):
        part = slice(q * chunk, (q + 1) * chunk)
        for direction in (1, -1):
            slot = me - direction * last

            @pl.when(jnp.logical_and(slot >= 0, slot < tp_size))
            def _():
                feature_copy(xg.at[slot], slot, q, direction).wait_recv()
                project_kv(slot, part)

        inv_rms = lax.rsqrt(sumsq[part, :] / (width * tp_size) + NORM_EPS)
        cosine = rot[0, part, :] * inv_rms
        sine = rot[1, part, :] * inv_rms
        rot[0, part, :] = cosine
        rot[1, part, :] = sine
        block = kvacc[part, :hw]
        turned = block * cosine + pltpu.roll(block, hw // 2, 1) * sine
        kvs[c, part, :hw] = turned.astype(BF16)
        kvs[c, part, hw:] = (kvacc[part, hw:] * inv_rms).astype(BF16)

        def send_kv(p, carry):
            kv_copy(c, q, p, kv_send.at[p, q]).start()
            return carry

        lax.fori_loop(c + 1, ctx_size, send_kv, 0)

    def rotate(block):
        return block * rot[0] + pltpu.roll(block, hw // 2, 1) * rot[1]

    project_q_hop(last)

    factor = math.log2(math.e) / math.sqrt(hw)
    lanes = rows
    groups = heads * share // lanes
    per_group = heads // groups
    for g in range(groups):
        turned = [
            rotate(qacc[:, h * hw:(h + 1) * hw]) * factor
            for h in range(g * per_group, (g + 1) * per_group)
        ]
        for part in range(tp_size):
            stacked = jnp.concatenate([t[part * share:(part + 1) * share] for t in turned], axis=0)
            qs[part, :, g * lanes:(g + 1) * lanes] = stacked.T.astype(BF16)

    def attend_own(part):
        key = lax.broadcasted_iota(jnp.int32, (rows, lanes), 0)
        row = lax.rem(lax.broadcasted_iota(jnp.int32, (rows, lanes), 1), share) + part * share
        allowed = key <= row
        k = kvs[c, :, :hw]
        vt = kvs[c, :, hw:].T
        for g in range(groups):
            at = slice(g * lanes, (g + 1) * lanes)
            scores = jnp.dot(k, qs[part, :, at], preferred_element_type=F32)
            scores = jnp.where(allowed, scores, MASKED)
            top = jnp.max(scores, axis=0, keepdims=True)
            expd = jnp.exp2(scores - top)
            high[:, at] = top
            total[:, at] = jnp.sum(expd, axis=0, keepdims=True)
            accum[:, at] = jnp.dot(vt, expd.astype(BF16), preferred_element_type=F32)

    def attend(part, slot):
        k = kvs[slot, :, :hw]
        vt = kvs[slot, :, hw:].T
        for g in range(groups):
            at = slice(g * lanes, (g + 1) * lanes)
            scores = jnp.dot(k, qs[part, :, at], preferred_element_type=F32)
            before = high[:, at]
            top = jnp.maximum(before, jnp.max(scores, axis=0, keepdims=True))
            shrink = jnp.exp2(before - top)
            expd = jnp.exp2(scores - top)
            high[:, at] = top
            total[:, at] = total[:, at] * shrink + jnp.sum(expd, axis=0, keepdims=True)
            accum[:, at] = accum[:, at] * shrink + jnp.dot(
                vt, expd.astype(BF16), preferred_element_type=F32
            )

    def attend_share(turn, carry):
        part = jnp.where(low, tp_size - 1 - turn, turn)
        first = turn == 0
        attend_own(part)

        def take(k, carry):
            slot = c - 1 - k

            @pl.when(first)
            def _():
                for q in range(ROW_CHUNKS):
                    kv_copy(slot, q, c, kv_send.at[c, q]).wait_recv()

            attend(part, slot)
            return carry

        lax.fori_loop(0, c, take, 0)

        out_rows = pl.ds(pl.multiple_of(part * share, share), share)
        for g in range(groups):
            at = slice(g * lanes, (g + 1) * lanes)
            turned = (accum[:, at] / total[:, at]).T.astype(BF16)
            for k in range(per_group):
                h = g * per_group + k
                att[out_rows, h * hw:(h + 1) * hw] = turned[k * share:(k + 1) * share]
        return carry

    low = me < tp_size // 2
    outer = jnp.logical_or(me == 0, me == tp_size - 1)

    copies[6].wait()
    columns = sbuf.shape[3]
    parts = sbuf.shape[1]

    def partial(d, n):
        return jnp.dot(
            att[pl.ds(pl.multiple_of(d * share, share), share), :],
            wo[:, pl.ds(pl.multiple_of(n * columns, columns), columns)],
            preferred_element_type=F32,
        )

    def sum_copy(d, n, direction):
        side = 0 if direction > 0 else 1
        return pltpu.make_async_remote_copy(
            src_ref=sbuf.at[d, n],
            dst_ref=rbuf.at[side, d, n],
            send_sem=rs_send.at[d, n],
            recv_sem=rs_recv.at[side, d, n],
            device_id={"tp": me + direction},
            device_id_type=MESH,
        )

    def phase(turn, carry):
        lax.fori_loop(
            jnp.where(outer, turn, jnp.minimum(turn, 1) * tp_size),
            jnp.where(outer, turn + 1, tp_size),
            attend_share,
            0,
        )

        def send_distance(k, carry):
            h = tp_size - 1 - k

            def send_part(n, carry):
                for direction, behind in ((1, has_dn), (-1, has_up)):
                    side = 0 if direction > 0 else 1
                    d = me + direction * h
                    inside = jnp.logical_and(d >= 0, d < tp_size)
                    now = jnp.where(outer, k == turn, turn == 0)

                    @pl.when(jnp.logical_and(inside, now))
                    def _():
                        fin[...] = partial(d, n)

                        @pl.when(behind)
                        def _():
                            sum_copy(d, n, direction).wait_recv()
                            fin[...] += rbuf[side, d, n].astype(F32)

                        sbuf[d, n] = fin[...].astype(BF16)
                        sum_copy(d, n, direction).start()

                return carry

            lax.fori_loop(0, parts, send_part, 0)
            return carry

        lax.fori_loop(0, tp_size - 1, send_distance, 0)
        return carry

    lax.fori_loop(0, tp_size, phase, 0)

    copies[7].wait()
    mine = pl.ds(pl.multiple_of(me * share, share), share)
    logit = jnp.zeros((share, 1), F32)
    for s in range(tp_size):
        logit += jnp.sum(
            xg[s, mine, :].astype(F32) * router_ref[:, s * width:(s + 1) * width],
            axis=1,
            keepdims=True,
        )
    gate = 1.0 / (1.0 + jnp.exp(-logit))

    for n in range(parts):
        fin[...] = partial(me, n)
        for direction, behind in ((1, has_dn), (-1, has_up)):
            side = 0 if direction > 0 else 1

            @pl.when(behind)
            def _():
                sum_copy(me, n, direction).wait_recv()
                fin[...] += rbuf[side, me, n].astype(F32)

        first = n * columns
        own = xg[first // width, mine, pl.ds(first % width, columns)].astype(F32)
        out_ref[:, first:first + columns] = (own + gate * fin[...]).astype(BF16)

    for direction, onward in ((1, has_up), (-1, has_dn)):
        for h in range(tp_size):
            slot = me - direction * h

            @pl.when(jnp.logical_and(jnp.logical_and(slot >= 0, slot < tp_size), onward))
            def _():
                for q in range(ROW_CHUNKS):
                    feature_copy(xg.at[slot], slot, q, direction).wait_send()

        for h in range(1, tp_size):
            d = me + direction * h

            @pl.when(jnp.logical_and(d >= 0, d < tp_size))
            def _():
                for n in range(parts):
                    sum_copy(d, n, direction).wait_send()

    def end_kv(p, carry):
        for q in range(ROW_CHUNKS):
            kv_copy(c, q, p, kv_send.at[p, q]).wait_send()
        return carry

    lax.fori_loop(c + 1, ctx_size, end_kv, 0)


def on_device(resid, sel_blocks, norm_gain, router_weight, w_query, w_key, value_projection, w_out):
    tp_size = lax.axis_size("tp")
    ctx_size = lax.axis_size("ctx")
    rows = sel_blocks.shape[0] * BLK
    local_rows, width = resid.shape
    total_blocks = local_rows // BLK * ctx_size
    freqs = np.exp(np.arange(HEAD_WIDTH // 2) * (-2.0 * math.log(ROPE_BASE) / HEAD_WIDTH))
    freqs = np.concatenate([freqs, freqs])[None, :]

    def table(positions):
        angles = positions[:, None] * freqs
        return jnp.asarray(np.concatenate([np.cos(angles), np.sin(angles)]).astype(np.float32))

    row_table = table(np.arange(BLK))
    block_table = table(np.arange(total_blocks) * BLK)

    smem = pl.BlockSpec(memory_space=pltpu.SMEM)
    picked, rotation = pl.pallas_call(
        pick,
        out_shape=(
            jax.ShapeDtypeStruct((rows, width), BF16),
            jax.ShapeDtypeStruct((2, rows, HEAD_WIDTH), F32),
        ),
        in_specs=[smem] + [pl.BlockSpec(memory_space=pl.ANY)] * 3,
        out_specs=(pl.BlockSpec(memory_space=pltpu.VMEM),) * 2,
        scratch_shapes=[
            pltpu.VMEM(row_table.shape, F32),
            pltpu.VMEM(block_table.shape, F32),
            pltpu.SemaphoreType.DMA((sel_blocks.shape[0] + 2,)),
        ],
        name="pick",
    )(
        sel_blocks, resid, row_table, block_table,
    )

    depth, q_width = w_query.shape
    out_width = w_out.shape[1]
    heads = q_width // HEAD_WIDTH
    share = rows // tp_size
    parts = out_width // width
    columns = width
    hw = HEAD_WIDTH
    vmem = pl.BlockSpec(memory_space=pltpu.VMEM)
    hbm = pl.BlockSpec(memory_space=pl.ANY)
    dma = pltpu.SemaphoreType.DMA
    return pl.pallas_call(
        functools.partial(fused, tp_size, ctx_size),
        out_shape=jax.ShapeDtypeStruct((share, out_width), BF16),
        in_specs=[hbm] * 8,
        out_specs=vmem,
        scratch_shapes=[
            pltpu.VMEM((2, rows, hw), F32),
            pltpu.VMEM((1, depth), F32),
            pltpu.VMEM((1, depth), F32),
            pltpu.VMEM((tp_size, rows, width), BF16),
            pltpu.VMEM(w_query.shape, BF16),
            pltpu.VMEM((depth, 2 * hw), BF16),
            pltpu.VMEM(w_out.shape, BF16),
            pltpu.VMEM((rows, q_width), F32),
            pltpu.VMEM((rows, 2 * hw), F32),
            pltpu.VMEM((rows, 1), F32),
            pltpu.VMEM((tp_size, hw, heads * share), BF16),
            pltpu.VMEM((ctx_size, rows, 2 * hw), BF16),
            pltpu.VMEM((1, heads * share), F32),
            pltpu.VMEM((1, heads * share), F32),
            pltpu.VMEM((hw, heads * share), F32),
            pltpu.VMEM((rows, q_width), BF16),
            pltpu.VMEM((tp_size, parts, share, columns), BF16),
            pltpu.VMEM((2, tp_size, parts, share, columns), BF16),
            pltpu.VMEM((share, columns), F32),
            dma((8,)),
            dma((2, tp_size, ROW_CHUNKS)),
            dma((tp_size, ROW_CHUNKS)),
            dma((ctx_size, ROW_CHUNKS)),
            dma((ctx_size, ROW_CHUNKS)),
            dma((tp_size, parts)),
            dma((2, tp_size, parts)),
        ],
        compiler_params=pltpu.CompilerParams(
            collective_id=0, has_side_effects=True, vmem_limit_bytes=60 * 1024 * 1024
        ),
        name="fused",
    )(
        picked, rotation,
        norm_gain.reshape(1, -1), router_weight.reshape(1, -1),
        w_query, w_key, value_projection, w_out,
    )


def solution(mesh):
    return jax.shard_map(
        on_device,
        mesh=mesh,
        in_specs=(
            P("ctx", "tp"),
            P("ctx"),
            P(),
            P(),
            P(None, "tp"),
            P(None, "tp"),
            P(None, "tp"),
            P("tp", None),
        ),
        out_specs=P(("ctx", "tp"), None),
        check_vma=False,
    )
```

```python
import functools
import math

import jax
import jax.numpy as jnp
import numpy as np
from jax import lax
from jax.experimental import pallas as pl
from jax.experimental.pallas import tpu as pltpu
from jax.sharding import PartitionSpec as P

HEAD_WIDTH = 128
BLK = 128
ROPE_BASE = 500000.0
NORM_EPS = 1e-05
MASKED = -1e30
MESH = pl.DeviceIdType.MESH
ROW_CHUNKS = 4
SHARED_PARTS = 2
BF16 = jnp.bfloat16
F32 = jnp.float32


def pick(sel_ref, resid_hbm, row_hbm, block_hbm, x_ref, rot, row_ref, block_ref, sem):
    picked = x_ref.shape[0] // BLK
    total_blocks = block_ref.shape[0] // 2
    before = lax.axis_index("ctx") * (resid_hbm.shape[0] // BLK)
    copies = [
        pltpu.make_async_copy(
            resid_hbm.at[pl.ds(pl.multiple_of((sel_ref[i] - before) * BLK, BLK), BLK), :],
            x_ref.at[pl.ds(i * BLK, BLK), :],
            sem.at[i],
        )
        for i in range(picked)
    ]
    tables = [
        pltpu.make_async_copy(src, dst, sem.at[picked + i])
        for i, (src, dst) in enumerate(((row_hbm, row_ref), (block_hbm, block_ref)))
    ]
    for copy in copies + tables:
        copy.start()
    for copy in tables:
        copy.wait()
    hw = HEAD_WIDTH
    flip = jnp.where(lax.broadcasted_iota(jnp.int32, (1, hw), 1) < hw // 2, -1.0, 1.0)
    for i in range(picked):
        part = slice(i * BLK, (i + 1) * BLK)
        block_cos = block_ref[pl.ds(sel_ref[i], 1), :]
        block_sin = block_ref[pl.ds(sel_ref[i] + total_blocks, 1), :]
        row_cos, row_sin = row_ref[:BLK, :], row_ref[BLK:, :]
        rot[0, part, :] = block_cos * row_cos - block_sin * row_sin
        rot[1, part, :] = (block_sin * row_cos + block_cos * row_sin) * flip
    for copy in copies:
        copy.wait()


def fused(
    tp_size, ctx_size,
    x_hbm, rot_hbm, gain_hbm, router_hbm, wq_hbm, wk_hbm, wv_hbm, wo_hbm,
    out_ref,
    rot, gain_ref, router_ref, xg, wq, wkv, wo, qacc, kvacc, sumsq, qs, kvs, high, total, accum, att,
    sbuf, rbuf, fin, wo_near, att_near,
    w_sem, ag_send, ag_recv, kv_send, kv_recv, rs_send, rs_recv,
    ship_send, ship_recv, spread_send, pair_send, att_send, att_recv,
):
    me = lax.axis_index("tp")
    c = lax.axis_index("ctx")
    rows, width = xg.shape[1:]
    heads = wq.shape[1] // HEAD_WIDTH
    hw = HEAD_WIDTH
    chunk = rows // ROW_CHUNKS
    share = rows // tp_size
    has_up = me < tp_size - 1
    has_dn = me > 0
    middle = jnp.logical_and(has_up, has_dn)
    end = jnp.logical_not(middle)
    inward = jnp.where(me == 0, 1, tp_size - 2)
    core = c % 2
    low_bit = c // 2 % 2
    high_bit = c // 4 % 2
    colour = (low_bit + high_bit) % 2
    other = c + 1 - 2 * core
    neighbours = (c + 2 - 4 * low_bit, c + 4 - 8 * high_bit)
    slab = wo.shape[0] // 8
    units = 2 * SHARED_PARTS
    columns = sbuf.shape[3]
    parts = sbuf.shape[1]
    split = parts - SHARED_PARTS

    copies = [
        pltpu.make_async_copy(src, dst, w_sem.at[i])
        for i, (src, dst) in enumerate(
            (
                (x_hbm, xg.at[me]),
                (gain_hbm, gain_ref),
                (wk_hbm, wkv.at[:, pl.ds(0, hw)]),
                (wv_hbm, wkv.at[:, pl.ds(hw, hw)]),
                (wq_hbm, wq),
                (rot_hbm, rot),
                (wo_hbm, wo),
                (router_hbm, router_ref),
            )
        )
    ]
    for copy in copies:
        copy.start()

    barrier = pltpu.get_barrier_semaphore()

    @pl.when(has_up)
    def _():
        pl.semaphore_signal(barrier, inc=1, device_id={"tp": me + 1}, device_id_type=MESH)

    @pl.when(has_dn)
    def _():
        pl.semaphore_signal(barrier, inc=1, device_id={"tp": me - 1}, device_id_type=MESH)

    def greet(k, carry):
        peer = lax.rem(c + k, ctx_size)
        pl.semaphore_signal(barrier, inc=1, device_id={"ctx": peer}, device_id_type=MESH)
        return carry

    lax.fori_loop(1, ctx_size, greet, 0)
    copies[0].wait()
    pl.semaphore_wait(
        barrier, ctx_size - 1 + has_up.astype(jnp.int32) + has_dn.astype(jnp.int32)
    )

    def piece_of(i, t, first=0):
        return (
            pl.ds(pl.multiple_of((2 * i + t % 2) * slab, slab), slab),
            pl.ds((t // 2 + first) * columns, columns),
        )

    own_slab = 2 * colour + core
    far_slab = 2 * (1 - colour) + core

    def ship_copy(t):
        return pltpu.make_async_remote_copy(
            src_ref=wo_hbm.at[piece_of(own_slab, t, split)],
            dst_ref=wo_near.at[piece_of(own_slab, t)],
            send_sem=ship_send.at[t],
            recv_sem=ship_recv.at[own_slab, t],
            device_id={"tp": inward},
            device_id_type=MESH,
        )

    def piece_copy(i, t, peer, send):
        return pltpu.make_async_remote_copy(
            src_ref=wo_near.at[piece_of(i, t)],
            dst_ref=wo_near.at[piece_of(i, t)],
            send_sem=send,
            recv_sem=ship_recv.at[i, t],
            device_id={"ctx": peer},
            device_id_type=MESH,
        )

    def spread_copy(t):
        return piece_copy(own_slab, t, neighbours[t // 2 % 2], spread_send.at[t])

    def spread(t):
        spread_copy(t).wait_recv()
        spread_copy(t).start()
        piece_copy(own_slab, t, other, pair_send.at[0, t]).start()

    def pass_on(t):
        copy = piece_copy(far_slab, t, other, pair_send.at[1, t])
        copy.wait_recv()
        copy.start()

    def have(n):
        for i in (2 * colour + 1 - core, 2 * (1 - colour) + 1 - core):
            for t in (2 * n, 2 * n + 1):
                piece_copy(i, t, other, pair_send.at[0, t]).wait_recv()

    def feature_copy(src, slot, q, direction):
        side = 0 if direction > 0 else 1
        part = pl.ds(q * chunk, chunk)
        return pltpu.make_async_remote_copy(
            src_ref=src.at[part, :],
            dst_ref=xg.at[slot, part, :],
            send_sem=ag_send.at[side, slot, q],
            recv_sem=ag_recv.at[slot, q],
            device_id={"tp": me + direction},
            device_id_type=MESH,
        )

    for q in range(ROW_CHUNKS):
        for direction, there in ((1, has_up), (-1, has_dn)):
            @pl.when(there)
            def _():
                feature_copy(xg.at[me], me, q, direction).start()

    @pl.when(end)
    def _():
        for t in range(units):
            ship_copy(t).start()

    sumsq[...] = jnp.zeros_like(sumsq)
    qacc[...] = jnp.zeros_like(qacc)
    kvacc[...] = jnp.zeros_like(kvacc)
    for i in (1, 2, 3):
        copies[i].wait()

    def project_kv(slot, part):
        depth = pl.ds(pl.multiple_of(slot * width, width), width)
        wide = xg[slot, part, :].astype(F32)
        sumsq[part, :] += jnp.sum(wide * wide, axis=1, keepdims=True)
        scaled = (wide * gain_ref[:, depth]).astype(BF16)
        kvacc[part, :] += jnp.dot(scaled, wkv[depth, :], preferred_element_type=F32)

    def project_q(slot):
        depth = pl.ds(pl.multiple_of(slot * width, width), width)
        scaled = (xg[slot].astype(F32) * gain_ref[:, depth]).astype(BF16)
        qacc[...] += jnp.dot(scaled, wq[depth, :], preferred_element_type=F32)

    def project_q_hop(h):
        for direction in (1, -1):
            slot = me - direction * h
            inside = jnp.logical_and(slot >= 0, slot < tp_size)

            @pl.when(jnp.logical_and(inside, jnp.logical_or(h > 0, direction > 0)))
            def _():
                project_q(slot)

    project_kv(me, slice(0, rows))
    copies[4].wait()
    halves = 2
    per_half = ROW_CHUNKS // halves

    def hop(h, carry):
        project_q_hop(h - 1)

        @pl.when(jnp.logical_and(middle, h == tp_size - 2))
        def _():
            spread(0)

        for q in range(ROW_CHUNKS):
            for direction, onward in ((1, has_up), (-1, has_dn)):
                slot = me - direction * h
                inside = jnp.logical_and(slot >= 0, slot < tp_size)

                @pl.when(inside)
                def _():
                    feature_copy(xg.at[slot], slot, q, direction).wait_recv()

                @pl.when(jnp.logical_and(inside, onward))
                def _():
                    feature_copy(xg.at[slot], slot, q, direction).start()

            if (q + 1) % per_half == 0:
                part = slice((q + 1 - per_half) * chunk, (q + 1) * chunk)
                for direction in (1, -1):
                    slot = me - direction * h

                    @pl.when(jnp.logical_and(slot >= 0, slot < tp_size))
                    def _():
                        project_kv(slot, part)

        return carry

    lax.fori_loop(1, tp_size - 1, hop, 0)
    project_q_hop(tp_size - 2)
    copies[5].wait()


    def kv_copy(slot, q, peer, send):
        part = pl.ds(q * chunk, chunk)
        return pltpu.make_async_remote_copy(
            src_ref=kvs.at[slot, part, :],
            dst_ref=kvs.at[slot, part, :],
            send_sem=send,
            recv_sem=kv_recv.at[slot, q],
            device_id={"ctx": peer},
            device_id_type=MESH,
        )

    last = tp_size - 1
    for q in range(ROW_CHUNKS):
        part = slice(q * chunk, (q + 1) * chunk)
        for direction in (1, -1):
            slot = me - direction * last

            @pl.when(jnp.logical_and(slot >= 0, slot < tp_size))
            def _():
                feature_copy(xg.at[slot], slot, q, direction).wait_recv()
                project_kv(slot, part)

        inv_rms = lax.rsqrt(sumsq[part, :] / (width * tp_size) + NORM_EPS)
        cosine = rot[0, part, :] * inv_rms
        sine = rot[1, part, :] * inv_rms
        rot[0, part, :] = cosine
        rot[1, part, :] = sine
        block = kvacc[part, :hw]
        turned = block * cosine + pltpu.roll(block, hw // 2, 1) * sine
        kvs[c, part, :hw] = turned.astype(BF16)
        kvs[c, part, hw:] = (kvacc[part, hw:] * inv_rms).astype(BF16)

        def send_kv(p, carry):
            kv_copy(c, q, p, kv_send.at[p, q]).start()
            return carry

        lax.fori_loop(c + 1, ctx_size, send_kv, 0)

    def rotate(block):
        return block * rot[0] + pltpu.roll(block, hw // 2, 1) * rot[1]

    @pl.when(middle)
    def _():
        spread(1)

    project_q_hop(last)

    factor = math.log2(math.e) / math.sqrt(hw)
    lanes = rows
    groups = heads * share // lanes
    per_group = heads // groups
    for g in range(groups):
        turned = [
            rotate(qacc[:, h * hw:(h + 1) * hw]) * factor
            for h in range(g * per_group, (g + 1) * per_group)
        ]
        for part in range(tp_size):
            stacked = jnp.concatenate([t[part * share:(part + 1) * share] for t in turned], axis=0)
            qs[part, :, g * lanes:(g + 1) * lanes] = stacked.T.astype(BF16)

    def attend(part, slot, count, opening):
        block = kvs[pl.ds(slot, count)].reshape(count * rows, 2 * hw)
        keys = block[:, :hw]
        vt = block[:, hw:].T
        if opening:
            key = lax.broadcasted_iota(jnp.int32, (rows, lanes), 0)
            row = lax.rem(lax.broadcasted_iota(jnp.int32, (rows, lanes), 1), share)
            allowed = key <= row + part * share
        for g in range(groups):
            at = slice(g * lanes, (g + 1) * lanes)
            scores = jnp.dot(keys, qs[part, :, at], preferred_element_type=F32)
            if opening:
                own = jnp.where(allowed, scores[(count - 1) * rows:], MASKED)
                if count > 1:
                    own = jnp.concatenate([scores[:(count - 1) * rows], own], axis=0)
                scores = own
            top = jnp.max(scores, axis=0, keepdims=True)
            if not opening:
                before = high[:, at]
                top = jnp.maximum(before, top)
            expd = jnp.exp2(scores - top)
            summed = jnp.sum(expd, axis=0, keepdims=True)
            mixed = jnp.dot(vt, expd.astype(BF16), preferred_element_type=F32)
            if not opening:
                shrink = jnp.exp2(before - top)
                summed = total[:, at] * shrink + summed
                mixed = accum[:, at] * shrink + mixed
            high[:, at] = top
            total[:, at] = summed
            accum[:, at] = mixed

    sizes = [size for size in (8, 4, 2, 1) if size <= ctx_size]
    opening = jnp.int32(1)
    for size in reversed(sizes):
        opening = jnp.where(c + 1 >= size, size, opening)
    rest = c + 1 - opening

    def attend_all(part):
        for size in sizes:
            @pl.when(opening == size)
            def _():
                attend(part, c + 1 - size, size, True)

        left = rest
        if ctx_size > sizes[0]:
            def one(k, carry):
                attend(part, rest - (k + 1) * sizes[0], sizes[0], False)
                return carry

            lax.fori_loop(0, rest // sizes[0], one, 0)
            left = lax.rem(rest, sizes[0])
        for size in sizes[1:]:
            if 2 * size < ctx_size:
                @pl.when(left >= size)
                def _():
                    attend(part, left - size, size, False)

                left = lax.rem(left, size)

    def attend_share(turn, carry):
        part = jnp.where(low, tp_size - 1 - turn, turn)
        first = turn == 0

        @pl.when(jnp.logical_and(middle, first))
        def _():
            spread(2)

        @pl.when(first)
        def _():
            def take(slot, carry):
                for q in range(ROW_CHUNKS):
                    kv_copy(slot, q, c, kv_send.at[c, q]).wait_recv()
                return carry

            lax.fori_loop(0, c, take, 0)

        attend_all(part)

        @pl.when(jnp.logical_and(middle, turn == 0))
        def _():
            spread(3)
            pass_on(0)
            pass_on(1)

        @pl.when(jnp.logical_and(middle, turn == tp_size - 2))
        def _():
            pass_on(2)

        out_rows = pl.ds(pl.multiple_of(part * share, share), share)
        for g in range(groups):
            at = slice(g * lanes, (g + 1) * lanes)
            turned = (accum[:, at] / total[:, at]).T.astype(BF16)
            for k in range(per_group):
                h = g * per_group + k
                att[out_rows, h * hw:(h + 1) * hw] = turned[k * share:(k + 1) * share]
        return carry

    low = me < tp_size // 2
    outer = jnp.logical_or(me == 0, me == tp_size - 1)

    copies[6].wait()

    def partial(d, n):
        return jnp.dot(
            att[pl.ds(pl.multiple_of(d * share, share), share), :],
            wo[:, pl.ds(pl.multiple_of(n * columns, columns), columns)],
            preferred_element_type=F32,
        )

    def sum_copy(d, n, direction):
        side = 0 if direction > 0 else 1
        return pltpu.make_async_remote_copy(
            src_ref=sbuf.at[d, n],
            dst_ref=rbuf.at[side, d, n],
            send_sem=rs_send.at[d, n],
            recv_sem=rs_recv.at[side, d, n],
            device_id={"tp": me + direction},
            device_id_type=MESH,
        )

    def att_copy(d, direction):
        return pltpu.make_async_remote_copy(
            src_ref=att.at[pl.ds(pl.multiple_of(d * share, share), share), :],
            dst_ref=att_near.at[d],
            send_sem=att_send.at[d],
            recv_sem=att_recv.at[d],
            device_id={"tp": me + direction},
            device_id_type=MESH,
        )

    def at_end(k):
        return jnp.logical_or(k == 0, k == tp_size - 1)

    def add_behind(d, n, direction, behind, shared, first):
        side = 0 if direction > 0 else 1
        near = jnp.logical_and(behind, jnp.logical_and(shared, at_end(me - direction)))

        @pl.when(near)
        def _():
            @pl.when(first)
            def _():
                att_copy(d, direction).wait_recv()

            cols = pl.ds(pl.multiple_of((n - split) * columns, columns), columns)
            fin[...] += jnp.dot(att_near[d], wo_near[:, cols], preferred_element_type=F32)

        @pl.when(jnp.logical_and(behind, jnp.logical_not(near)))
        def _():
            sum_copy(d, n, direction).wait_recv()
            fin[...] += rbuf[side, d, n].astype(F32)

    def phase(turn, carry):
        lax.fori_loop(
            jnp.where(outer, turn, jnp.minimum(turn, 1) * tp_size),
            jnp.where(outer, turn + 1, tp_size),
            attend_share,
            0,
        )


        def send_distance(k, carry):
            h = tp_size - 1 - k

            def send_part(n, carry):
                opening_part = jnp.logical_and(middle, jnp.logical_and(turn == 0, k == 1))

                @pl.when(jnp.logical_and(opening_part, n == 1))
                def _():
                    pass_on(units - 1)

                for i in range(SHARED_PARTS):
                    @pl.when(jnp.logical_and(opening_part, n == split + i))
                    def _():
                        have(i)

                for direction, behind in ((1, has_dn), (-1, has_up)):
                    d = me + direction * h
                    inside = jnp.logical_and(d >= 0, d < tp_size)
                    now = jnp.logical_and(inside, jnp.where(outer, k == turn, turn == 0))
                    shared = n >= split

                    @pl.when(jnp.logical_and(now, jnp.logical_and(end, n == split)))
                    def _():
                        att_copy(d, direction).start()

                    @pl.when(jnp.logical_and(now, jnp.logical_or(middle, n < split)))
                    def _():
                        fin[...] = partial(d, n)
                        add_behind(d, n, direction, behind, shared, n == split)
                        sbuf[d, n] = fin[...].astype(BF16)
                        sum_copy(d, n, direction).start()

                return carry

            lax.fori_loop(0, parts, send_part, 0)
            return carry

        lax.fori_loop(0, tp_size - 1, send_distance, 0)
        return carry

    lax.fori_loop(0, tp_size, phase, 0)

    copies[7].wait()
    mine = pl.ds(pl.multiple_of(me * share, share), share)
    logit = jnp.zeros((share, 1), F32)
    for s in range(tp_size):
        logit += jnp.sum(
            xg[s, mine, :].astype(F32) * router_ref[:, s * width:(s + 1) * width],
            axis=1,
            keepdims=True,
        )
    gate = 1.0 / (1.0 + jnp.exp(-logit))

    for n in range(parts):
        fin[...] = partial(me, n)
        for direction, behind in ((1, has_dn), (-1, has_up)):
            add_behind(me, n, direction, behind, n >= split, n == split)

        first = n * columns
        own = xg[first // width, mine, pl.ds(first % width, columns)].astype(F32)
        out_ref[:, first:first + columns] = (own + gate * fin[...]).astype(BF16)

    for direction, onward in ((1, has_up), (-1, has_dn)):
        for h in range(tp_size):
            slot = me - direction * h

            @pl.when(jnp.logical_and(jnp.logical_and(slot >= 0, slot < tp_size), onward))
            def _():
                for q in range(ROW_CHUNKS):
                    feature_copy(xg.at[slot], slot, q, direction).wait_send()

        for h in range(1, tp_size):
            d = me + direction * h

            @pl.when(jnp.logical_and(d >= 0, d < tp_size))
            def _():
                for n in range(split):
                    sum_copy(d, n, direction).wait_send()

                @pl.when(middle)
                def _():
                    for n in range(split, parts):
                        sum_copy(d, n, direction).wait_send()

                @pl.when(end)
                def _():
                    att_copy(d, direction).wait_send()

    def end_kv(p, carry):
        for q in range(ROW_CHUNKS):
            kv_copy(c, q, p, kv_send.at[p, q]).wait_send()
        return carry

    lax.fori_loop(c + 1, ctx_size, end_kv, 0)

    @pl.when(end)
    def _():
        for t in range(units):
            ship_copy(t).wait_send()

    @pl.when(middle)
    def _():
        for t in range(units):
            spread_copy(t).wait_send()
            piece_copy(own_slab, t, other, pair_send.at[0, t]).wait_send()
            piece_copy(far_slab, t, other, pair_send.at[1, t]).wait_send()


def on_device(resid, sel_blocks, norm_gain, router_weight, w_query, w_key, value_projection, w_out):
    tp_size = lax.axis_size("tp")
    ctx_size = lax.axis_size("ctx")
    rows = sel_blocks.shape[0] * BLK
    local_rows, width = resid.shape
    total_blocks = local_rows // BLK * ctx_size
    freqs = np.exp(np.arange(HEAD_WIDTH // 2) * (-2.0 * math.log(ROPE_BASE) / HEAD_WIDTH))
    freqs = np.concatenate([freqs, freqs])[None, :]

    def table(positions):
        angles = positions[:, None] * freqs
        return jnp.asarray(np.concatenate([np.cos(angles), np.sin(angles)]).astype(np.float32))

    row_table = table(np.arange(BLK))
    block_table = table(np.arange(total_blocks) * BLK)

    smem = pl.BlockSpec(memory_space=pltpu.SMEM)
    picked, rotation = pl.pallas_call(
        pick,
        out_shape=(
            jax.ShapeDtypeStruct((rows, width), BF16),
            jax.ShapeDtypeStruct((2, rows, HEAD_WIDTH), F32),
        ),
        in_specs=[smem] + [pl.BlockSpec(memory_space=pl.ANY)] * 3,
        out_specs=(pl.BlockSpec(memory_space=pltpu.VMEM),) * 2,
        scratch_shapes=[
            pltpu.VMEM(row_table.shape, F32),
            pltpu.VMEM(block_table.shape, F32),
            pltpu.SemaphoreType.DMA((sel_blocks.shape[0] + 2,)),
        ],
        name="pick",
    )(
        sel_blocks, resid, row_table, block_table,
    )

    depth, q_width = w_query.shape
    out_width = w_out.shape[1]
    heads = q_width // HEAD_WIDTH
    share = rows // tp_size
    parts = out_width // width
    columns = width
    hw = HEAD_WIDTH
    vmem = pl.BlockSpec(memory_space=pltpu.VMEM)
    hbm = pl.BlockSpec(memory_space=pl.ANY)
    dma = pltpu.SemaphoreType.DMA
    return pl.pallas_call(
        functools.partial(fused, tp_size, ctx_size),
        out_shape=jax.ShapeDtypeStruct((share, out_width), BF16),
        in_specs=[hbm] * 8,
        out_specs=vmem,
        scratch_shapes=[
            pltpu.VMEM((2, rows, hw), F32),
            pltpu.VMEM((1, depth), F32),
            pltpu.VMEM((1, depth), F32),
            pltpu.VMEM((tp_size, rows, width), BF16),
            pltpu.VMEM(w_query.shape, BF16),
            pltpu.VMEM((depth, 2 * hw), BF16),
            pltpu.VMEM(w_out.shape, BF16),
            pltpu.VMEM((rows, q_width), F32),
            pltpu.VMEM((rows, 2 * hw), F32),
            pltpu.VMEM((rows, 1), F32),
            pltpu.VMEM((tp_size, hw, heads * share), BF16),
            pltpu.VMEM((ctx_size, rows, 2 * hw), BF16),
            pltpu.VMEM((1, heads * share), F32),
            pltpu.VMEM((1, heads * share), F32),
            pltpu.VMEM((hw, heads * share), F32),
            pltpu.VMEM((rows, q_width), BF16),
            pltpu.VMEM((tp_size, parts, share, columns), BF16),
            pltpu.VMEM((2, tp_size, parts, share, columns), BF16),
            pltpu.VMEM((share, columns), F32),
            pltpu.VMEM((w_out.shape[0], SHARED_PARTS * columns), BF16),
            pltpu.VMEM((tp_size, share, q_width), BF16),
            dma((8,)),
            dma((2, tp_size, ROW_CHUNKS)),
            dma((tp_size, ROW_CHUNKS)),
            dma((ctx_size, ROW_CHUNKS)),
            dma((ctx_size, ROW_CHUNKS)),
            dma((tp_size, parts)),
            dma((2, tp_size, parts)),
            dma((2 * SHARED_PARTS,)),
            dma((4, 2 * SHARED_PARTS)),
            dma((2 * SHARED_PARTS,)),
            dma((2, 2 * SHARED_PARTS)),
            dma((tp_size,)),
            dma((tp_size,)),
        ],
        compiler_params=pltpu.CompilerParams(
            collective_id=0, has_side_effects=True, vmem_limit_bytes=60 * 1024 * 1024
        ),
        name="fused",
    )(
        picked, rotation,
        norm_gain.reshape(1, -1), router_weight.reshape(1, -1),
        w_query, w_key, value_projection, w_out,
    )


def solution(mesh):
    return jax.shard_map(
        on_device,
        mesh=mesh,
        in_specs=(
            P("ctx", "tp"),
            P("ctx"),
            P(),
            P(),
            P(None, "tp"),
            P(None, "tp"),
            P(None, "tp"),
            P("tp", None),
        ),
        out_specs=P(("ctx", "tp"), None),
        check_vma=False,
    )
```
